32 devices in a mesh: ctx: 8 (over z, y), kvh: 4 (over x, core).
Axes of the slice: x: 2, y: 2, z: 4, core: 2. Of those that a mesh axis runs over, the one named last changes fastest.
Arguments:
- queries: bfloat16 [2048, 2048], P(('ctx', 'kvh')), may hold values from -42 to 42
- keys: bfloat16 [2048, 512], P(('ctx', 'kvh')), may hold values from -6 to 6
- values: bfloat16 [2048, 512], P(('ctx', 'kvh')), may hold values from -6 to 6
- doc_lengths: int32 [16], replicated, may hold values from 1 to 1024, 2048 in all
Outputs:
- attended: bfloat16 [2048, 2048], P(('ctx', 'kvh'))
The draws below stay inside these ranges and needn't reach their ends.
Inputs may be any that keep to these rules, and one draw needn't show every extreme that they name: `doc_lengths`: positive lengths that sum to 2048.
All inputs are finite; a program needn't handle non-finite values.
Results may differ from the reference program's by a relative error of at most 0.005.
Values may be sent and summed in bfloat16 or wider, within the bound.
A program may use at most 64 MiB of HBM per device.

```python
import math
import jax
import jax.numpy as jnp
import numpy as np
from jax import lax

QUERY_HEADS = 16
KEY_VALUE_HEADS = 4
HEAD_SIZE = 128
SINK = 128
DOCS = 16
PACKED_LENGTH = 2048


def shared_sink_keys(key):
    base_offset = jnp.clip(jax.random.normal(jax.random.fold_in(key, 11), (PACKED_LENGTH, KEY_VALUE_HEADS * HEAD_SIZE), jnp.float32), -6.0, 6.0)
    return base_offset


def draw_keys(key, part):
    return shared_sink_keys(key).astype(jnp.bfloat16)


def draw_queries(key, part):
    base_offset = jnp.clip(jax.random.normal(jax.random.fold_in(key, 23), (PACKED_LENGTH, QUERY_HEADS * HEAD_SIZE), jnp.float32), -6.0, 6.0)
    return base_offset.astype(jnp.bfloat16)


def steps_of(rng, extent, cuts, smallest, largest):
    factor_of = 1.0
    for dim, shards_of in cuts:
        heights = jax.random.uniform(jax.random.fold_in(jax.random.fold_in(rng, 6), dim), (shards_of,), jnp.float32, smallest / len(cuts), largest / len(cuts))
        factor_of = factor_of * jnp.repeat(jnp.exp(heights), extent[dim] // shards_of).reshape((-1,) + (1,) * (len(extent) - 1 - dim))
    return factor_of


def profile(count, total, most, skew):
    portions = [(1 << 20) // math.isqrt(grade ** skew) + 1 for grade in range(2, count + 1)]
    spare, counts = total - most - (count - 1), [1] * (count - 1)
    while spare > 0:
        candidates = [i for i in range(count - 1) if counts[i] < most]
        whole, left = sum([portions[i] for i in candidates]), spare
        for i in candidates:
            more = min(most - counts[i], max(1, left * portions[i] // whole), spare)
            counts[i] = counts[i] + more
            spare = spare - more
    return np.array([most] + counts)


def uneven_parts(stream_key, number_of, total, reach, lean):
    if number_of == 2:
        one = jax.random.randint(stream_key, (), max(1, total - reach), min(reach, total - 1) + 1)
        return jnp.stack([one, total - one])
    sizes = jnp.asarray(profile(number_of, total, reach, lean), jnp.int32)
    pairs = (number_of - 1) // 2
    donor, receiver = sizes[1:1 + 2 * pairs:2], sizes[2:2 + 2 * pairs:2]
    room = jnp.minimum(donor - 1, reach - receiver)
    shifted = jax.random.randint(jax.random.fold_in(stream_key, 1), (pairs,), 0, 1 << 20) % (room + 1)
    sizes = sizes.at[1:1 + 2 * pairs:2].set(donor - shifted).at[2:2 + 2 * pairs:2].set(receiver + shifted)
    return sizes[jax.random.permutation(jax.random.fold_in(stream_key, 2), number_of)]


def scatter_about(own_key, extent, width, reach, cuts=(), kind=jnp.bfloat16):
    loudness = steps_of(own_key, extent, cuts, -0.22, 0.18) if cuts else 1.0
    drawn = jax.random.normal(own_key, extent, jnp.float32) * width * loudness
    return jnp.minimum(jnp.maximum(drawn, -reach), reach).astype(kind)


def setup_inputs(seed: int = 0) -> dict:
    arg_keys = jax.random.split(jax.random.key(seed), 5)
    queries = draw_queries(jax.random.fold_in(arg_keys[4], 71), 0)
    keys = draw_keys(jax.random.fold_in(arg_keys[4], 71), 0)
    values = scatter_about(arg_keys[2], (PACKED_LENGTH, KEY_VALUE_HEADS * HEAD_SIZE), 1.0, 6.0, ((0, 32),))
    doc_lengths = uneven_parts(arg_keys[3], DOCS, PACKED_LENGTH, PACKED_LENGTH // 2, 2).astype(jnp.int32)
    return {"queries": queries, "keys": keys, "values": values, "doc_lengths": doc_lengths}


def reference(queries, keys, values, doc_lengths):
    packed_sequence = queries.shape[0]
    pos = jnp.arange(packed_sequence, dtype=jnp.int32)
    starts = jnp.cumsum(doc_lengths) - doc_lengths
    doc = jnp.sum((pos[:, None] >= starts[None, :]).astype(jnp.int32), axis=1)
    allowed = (pos[None, :] <= pos[:, None]) & ((doc[:, None] == doc[None, :]) | (pos[None, :] < SINK))
    query_heads = queries.reshape(packed_sequence, QUERY_HEADS, HEAD_SIZE)
    key_head_rows = keys.reshape(packed_sequence, KEY_VALUE_HEADS, HEAD_SIZE)
    value_head_rows = values.reshape(packed_sequence, KEY_VALUE_HEADS, HEAD_SIZE)
    query_group = QUERY_HEADS // KEY_VALUE_HEADS
    scale = HEAD_SIZE ** -0.5

    def one_head(head):
        q_head = query_heads[:, head]
        k_head = key_head_rows[:, head // query_group]
        v_head = value_head_rows[:, head // query_group]
        scores = jnp.dot(q_head, k_head.T, preferred_element_type=jnp.float32) * scale
        scores = jnp.where(allowed, scores, jnp.float32(-1e30))
        rowmax = jnp.max(scores, axis=1, keepdims=True)
        expo = jnp.where(allowed, jnp.exp(scores - rowmax), jnp.float32(0.0))
        total = jnp.sum(expo, axis=1, keepdims=True)
        weights = expo.astype(jnp.bfloat16)
        return jnp.dot(weights, v_head, preferred_element_type=jnp.float32) / total

    result = lax.map(one_head, jnp.arange(QUERY_HEADS, dtype=jnp.int32))
    return jnp.transpose(result, (1, 0, 2)).reshape(packed_sequence, QUERY_HEADS * HEAD_SIZE).astype(jnp.bfloat16)
```

```python
import functools
import math

import jax
import jax.numpy as jnp
from jax import lax
from jax.experimental import pallas as pl
from jax.experimental.pallas import tpu as pltpu
from jax.sharding import PartitionSpec as P

HEAD_SIZE = 128
SINK = 128
NEG = -1e30


def attention_kernel(
    planes, reach, kv_heads, group,
    lens_ref, q_hbm, k_hbm, v_hbm, o_ref,
    kbuf, vbuf, qbuf, scores, bias,
    local_sem, send_sem, recv_sem, pair_send, pair_recv, sink_send,
):
    rows = k_hbm.shape[0]
    chip = 2 * rows
    plane = 4 * chip
    ctx, kvh = lax.axis_index("ctx"), lax.axis_index("kvh")
    z, y = ctx // 2, ctx % 2
    x, core = kvh // 2, kvh % 2
    col = 2 * y + x
    xcol, ycol, dcol = 2 * y + 1 - x, 2 * (1 - y) + x, 3 - col
    even = x == y
    bufs = (kbuf, vbuf)

    def dev(xx, yy, zz, cc):
        return (2 * zz + yy, 2 * xx + cc)

    to_x, to_y, partner = dev(1 - x, y, z, core), dev(x, 1 - y, z, core), dev(x, y, z, 1 - core)
    to_z = dev(x, y, z + 1, core)

    names = ["own", "S"] + [("Z", d) for d in range(1, reach + 1)]
    names += [("F", d, w) for d in range(1, reach) for w in "XYD"] + [("M", w) for w in "XYD"]
    index = {name: n for n, name in enumerate(names)}

    def at(slot, column, cc=None):
        return slot * plane + column * chip + (core if cc is None else cc) * rows

    def extra(which, cc=None):
        return reach * plane + which * chip + (core if cc is None else cc) * rows

    def view(t, start):
        return bufs[t].at[pl.ds(pl.multiple_of(start, rows), rows), :]

    finals = []

    def send(t, name, src, dst, device, cond):
        n = index[name]

        def make():
            return pltpu.make_async_remote_copy(
                src_ref=view(t, src), dst_ref=view(t, dst),
                send_sem=send_sem.at[t, n], recv_sem=recv_sem.at[t, n],
                device_id=device, device_id_type=pl.DeviceIdType.MESH,
            )

        @pl.when(cond)
        def _():
            make().start()

        finals.append((cond, make))

    def pair_copy(t, name, start, sem_only=False):
        n = index[name]
        return pltpu.make_async_remote_copy(
            src_ref=view(t, start), dst_ref=view(t, start),
            send_sem=pair_send.at[t, n], recv_sem=pair_recv.at[t, n],
            device_id=partner, device_id_type=pl.DeviceIdType.MESH,
        )

    pair_waits = ([], [])

    def arrive(t, name, start, other, cond):
        n = index[name]

        @pl.when(cond)
        def _():
            pltpu.make_async_remote_copy(
                src_ref=view(t, start), dst_ref=view(t, start),
                send_sem=send_sem.at[t, n], recv_sem=recv_sem.at[t, n],
                device_id=partner, device_id_type=pl.DeviceIdType.MESH,
            ).wait_recv()
            pair_copy(t, name, start).start()

        finals.append((cond, lambda: pair_copy(t, name, start)))
        pair_waits[t].append((cond, name, other))

    def both(start_of):
        return start_of(core), start_of(1 - core)

    def send_sinks(t, cond):
        for number in range(reach, planes):
            def make(number=number):
                return pltpu.make_async_remote_copy(
                    src_ref=view(t, at(0, 0)), dst_ref=view(t, extra(1)),
                    send_sem=sink_send.at[t, number], recv_sem=recv_sem.at[t, index["S"]],
                    device_id=dev(x, y, number, core), device_id_type=pl.DeviceIdType.MESH,
                )

            @pl.when(cond)
            def _():
                make().start()

            finals.append((cond, make))

    true = z >= 0

    def own(t):
        pltpu.make_async_copy((k_hbm, v_hbm)[t], view(t, at(0, col)), local_sem.at[t]).wait()
        send(t, ("Z", 1), at(0, col), at(1, col) if reach > 1 else extra(0), to_z, z + 1 < planes)
        send(t, ("M", "X"), at(0, col), at(0, col), to_x, xcol > col)
        send(t, ("M", "Y"), at(0, col), at(0, col), to_y, ycol > col)
        pair_copy(t, "own", at(0, col)).start()
        finals.append((true, lambda: pair_copy(t, "own", at(0, col))))
        pair_waits[t].append((true, "own", at(0, col, 1 - core)))
        send_sinks(t, (z == 0) & (col == 0))

    def column(t, d):
        start_of = (lambda cc: at(d, col, cc)) if d < reach else (lambda cc: extra(0, cc))
        here, other = both(start_of)
        arrive(t, ("Z", d), here, other, z >= d)
        if d < reach:
            send(t, ("Z", d + 1), here, at(d + 1, col) if d + 1 < reach else extra(0), to_z,
                 (z >= d) & (z + 1 < planes))
            send(t, ("F", d, "X"), here, here, to_x, z >= d)
            send(t, ("F", d, "Y"), here, here, to_y, z >= d)
        else:
            send(t, ("M", "X"), here, at(0, col), to_x, (z >= d) & (xcol < col))
            send(t, ("M", "Y"), here, at(0, col), to_y, (z >= d) & (ycol < col))

    def relay_m(t, cond):
        source = jnp.where(even, ycol, xcol)
        device = dev(jnp.where(even, 1 - x, x), jnp.where(even, y, 1 - y), z, core)
        send(t, ("M", "D"), at(0, source), at(0, source), device, cond(source, 3 - source))

    def mixed_early(t):
        for w, j in (("X", xcol), ("Y", ycol)):
            arrive(t, ("M", w), *both(lambda cc, j=j: at(0, j, cc)), j < col)
        relay_m(t, lambda s, d: s < d)
        send_sinks(t, (z == 0) & ((col == 1) | (col == 2)))

    def mixed_late(t):
        for w, j in (("X", xcol), ("Y", ycol)):
            arrive(t, ("M", w), *both(lambda cc, j=j: at(0, j, cc)), (j > col) & (z >= reach))
        relay_m(t, lambda s, d: (s > d) & (z >= reach))

    def mixed_diag(t, late):
        cond = ((dcol > col) & (z >= reach)) if late else (dcol < col)
        arrive(t, ("M", "D"), *both(lambda cc: at(0, dcol, cc)), cond)
        if not late:
            send_sinks(t, (z == 0) & (col == 3))

    def full(t, d):
        for w, j in (("X", xcol), ("Y", ycol)):
            arrive(t, ("F", d, w), *both(lambda cc, j=j: at(d, j, cc)), z >= d)
        source = jnp.where(even, xcol, ycol)
        device = dev(jnp.where(even, x, 1 - x), jnp.where(even, 1 - y, y), z, core)
        send(t, ("F", d, "D"), at(d, source), at(d, source), device, z >= d)

    def full_diag(t, d):
        arrive(t, ("F", d, "D"), *both(lambda cc: at(d, dcol, cc)), z >= d)

    def sink(t):
        arrive(t, "S", *both(lambda cc: extra(1, cc)), z >= reach)

    def from_pair(t):
        for cond, name, other in pair_waits[t]:
            @pl.when(cond)
            def _():
                pair_copy(t, name, other).wait_recv()

    pltpu.make_async_copy(k_hbm, view(0, at(0, col)), local_sem.at[0]).start()
    pltpu.make_async_copy(v_hbm, view(1, at(0, col)), local_sem.at[1]).start()
    q_copy = pltpu.make_async_copy(q_hbm, qbuf, local_sem.at[2])
    q_copy.start()
    barrier = pltpu.get_barrier_semaphore()
    for device in (to_x, to_y, partner):
        pl.semaphore_signal(barrier, inc=1, device_id=device, device_id_type=pl.DeviceIdType.MESH)
    for step in range(1, planes):
        pl.semaphore_signal(
            barrier, inc=1, device_id=dev(x, y, (z + step) % planes, core),
            device_id_type=pl.DeviceIdType.MESH,
        )
    pl.semaphore_wait(barrier, planes + 2)

    own(0)
    own(1)

    def clear(start, count, cond):
        @pl.when(cond)
        def _():
            for buf in bufs:
                buf[start:start + count, :] = jnp.zeros((count, buf.shape[1]), buf.dtype)

    for d in range(1, reach):
        clear(d * plane, plane, z < d)
    for j in range(1, 4):
        clear(j * chip, chip, (j > col) & (z < reach))
    clear(reach * plane, 2 * chip, z < reach)

    q_pos = ctx * (4 * rows) + kvh * rows + lax.broadcasted_iota(jnp.int32, (rows, 1), 0)
    first = jnp.zeros((rows, 1), jnp.int32)
    begin = jnp.int32(0)
    for n in range(lens_ref.shape[0]):
        first = jnp.where(q_pos >= begin, begin, first)
        begin = begin + lens_ref[n]
    lane = lax.broadcasted_iota(jnp.int32, (1, chip), 1)

    def set_bias(start, base):
        k_pos = base + lane
        sees = (k_pos <= q_pos) & ((k_pos >= first) | ((k_pos < SINK) & (k_pos >= 0)))
        bias[:, start:start + chip] = jnp.where(sees, jnp.float32(0.0), jnp.float32(NEG))

    nowhere = -planes * plane * 2
    for j in range(4):
        set_bias(j * chip, jnp.where(j <= col, z, z - reach) * plane + j * chip)
        for d in range(1, reach):
            set_bias(d * plane + j * chip, (z - d) * plane + j * chip)
    set_bias(reach * plane, (z - reach) * plane + col * chip)
    set_bias(reach * plane + chip, jnp.where((z > reach) | ((z == reach) & (col > 0)), 0, nowhere))

    def arrivals(t, part):
        if part == 0:
            column(t, 1)
            mixed_early(t)
        elif part == 1:
            for d in range(2, reach + 1):
                column(t, d)
            for d in range(1, reach):
                full(t, d)
            mixed_diag(t, False)
        else:
            mixed_late(t)

    def last(t):
        for d in range(1, reach):
            full_diag(t, d)
        sink(t)
        mixed_diag(t, True)

    for part in range(3):
        for t in range(2):
            arrivals(t, part)
    last(0)
    from_pair(0)
    q_copy.wait()

    keys = bias.shape[1]
    step = 2 * chip
    tall = group * rows
    size = HEAD_SIZE

    def head_q(h):
        return jnp.concatenate(
            [qbuf[:, (h * group + g) * size:(h * group + g + 1) * size] for g in range(group)], axis=0
        )

    def fold(op, value, total):
        for n in range(value.shape[1] // size):
            total = op(total, value[:, n * size:(n + 1) * size])
        return total

    def each(body, init):
        count = keys // step
        if count <= 8:
            for n in range(count):
                init = body(n, init)
            return init
        return lax.fori_loop(0, count, body, init)

    def cut(n):
        return pl.ds(n * step if isinstance(n, int) else pl.multiple_of(n * step, step), step)

    tops = []
    for h in range(kv_heads):
        qh = head_q(h)

        def score(n, top, h=h, qh=qh):
            s = lax.dot_general(
                qh, kbuf[cut(n), h * size:(h + 1) * size], (((1,), (1,)), ((), ())),
                preferred_element_type=jnp.float32,
            )
            s = s + jnp.concatenate([bias[:, cut(n)]] * group, axis=0)
            scores[h * tall:(h + 1) * tall, cut(n)] = s
            return fold(jnp.maximum, s, top)

        top = each(score, jnp.full((tall, size), NEG, jnp.float32))
        tops.append(jnp.max(top, axis=1, keepdims=True))

    last(1)
    from_pair(1)

    factor = jnp.float32(HEAD_SIZE ** -0.5 * math.log2(math.e))
    for h in range(kv_heads):
        def weigh(n, carry, h=h):
            total, acc = carry
            p = jnp.exp2((scores[h * tall:(h + 1) * tall, cut(n)] - tops[h]) * factor)
            acc = acc + jnp.dot(
                p.astype(jnp.bfloat16), vbuf[cut(n), h * size:(h + 1) * size],
                preferred_element_type=jnp.float32,
            )
            return fold(jnp.add, p, total), acc

        zero = jnp.zeros((tall, size), jnp.float32)
        total, acc = each(weigh, (zero, zero))
        out = (acc / jnp.sum(total, axis=1, keepdims=True)).astype(o_ref.dtype)
        for g in range(group):
            o_ref[:, (h * group + g) * size:(h * group + g + 1) * size] = out[g * rows:(g + 1) * rows]

    for cond, make in finals:
        @pl.when(cond)
        def _():
            make().wait_send()


def solution(mesh):
    planes = mesh.shape["ctx"] // 2
    reach = planes // 2

    def shards(queries, keys, values, doc_lengths):
        rows, width = keys.shape
        kv_heads = width // HEAD_SIZE
        group = queries.shape[1] // width
        span = (4 * reach + 2) * 2 * rows
        pieces = 2 + reach + 3 * (reach - 1) + 3
        return pl.pallas_call(
            functools.partial(attention_kernel, planes, reach, kv_heads, group),
            out_shape=jax.ShapeDtypeStruct(queries.shape, queries.dtype),
            in_specs=[pl.BlockSpec(memory_space=pltpu.SMEM)] + [pl.BlockSpec(memory_space=pl.ANY)] * 3,
            out_specs=pl.BlockSpec(memory_space=pltpu.VMEM),
            scratch_shapes=[
                pltpu.VMEM((span, width), keys.dtype),
                pltpu.VMEM((span, width), values.dtype),
                pltpu.VMEM(queries.shape, queries.dtype),
                pltpu.VMEM((kv_heads * group * rows, span), jnp.float32),
                pltpu.VMEM((rows, span), jnp.float32),
                pltpu.SemaphoreType.DMA((3,)),
                pltpu.SemaphoreType.DMA((2, pieces)),
                pltpu.SemaphoreType.DMA((2, pieces)),
                pltpu.SemaphoreType.DMA((2, pieces)),
                pltpu.SemaphoreType.DMA((2, pieces)),
                pltpu.SemaphoreType.DMA((2, planes)),
            ],
            compiler_params=pltpu.CompilerParams(
                collective_id=0, has_side_effects=True, vmem_limit_bytes=64 * 1024 * 1024 - 65536,
            ),
            name="attend",
        )(doc_lengths, queries, keys, values)

    placed = (P(("ctx", "kvh"), None), P(("ctx", "kvh"), None), P(("ctx", "kvh"), None), P())
    return jax.shard_map(
        shards, mesh=mesh, in_specs=placed, out_specs=P(("ctx", "kvh"), None), check_vma=False
    )
```

```python
import functools
import math

import jax
import jax.numpy as jnp
from jax import lax
from jax.experimental import pallas as pl
from jax.experimental.pallas import tpu as pltpu
from jax.sharding import PartitionSpec as P

HEAD_SIZE = 128
SINK = 128
NEG = -1e30
CHUNKS = 1


def attention_kernel(
    planes, reach, kv_heads, group,
    lens_hbm, q_hbm, k_hbm, v_hbm, o_ref,
    lens_ref, kbuf, vbuf, qbuf, scores, bias,
    local_sem, send_sem, recv_sem, pair_send, pair_recv, far_send,
):
    rows = k_hbm.shape[0]
    chip = 2 * rows
    plane = 4 * chip
    ctx, kvh = lax.axis_index("ctx"), lax.axis_index("kvh")
    z, y = ctx // 2, ctx % 2
    x, core = kvh // 2, kvh % 2
    col = 2 * y + x
    xcol, ycol, dcol = 2 * y + 1 - x, 2 * (1 - y) + x, 3 - col
    bufs = (kbuf, vbuf)

    def dev(xx, yy, zz, cc):
        return (2 * zz + yy, 2 * xx + cc)

    to_x, to_y, partner = dev(1 - x, y, z, core), dev(x, 1 - y, z, core), dev(x, y, z, 1 - core)
    to_d = dev(1 - x, 1 - y, z, core)
    ways = (("X", to_x, xcol), ("Y", to_y, ycol), ("D", to_d, dcol))

    names = ["own", "S"] + [("Z", d) for d in range(1, reach + 1)]
    names += [("F", d, w) for d in range(1, reach) for w in "XYD"] + [("M", w) for w in "XYD"]
    index = {name: n for n, name in enumerate(names)}

    def at(slot, column, cc=None):
        return slot * plane + column * chip + (core if cc is None else cc) * rows

    def extra(which, cc=None):
        return reach * plane + which * chip + (core if cc is None else cc) * rows

    part = rows // CHUNKS

    def view(t, start):
        first = start + (t % CHUNKS) * part
        return bufs[t // CHUNKS].at[pl.ds(pl.multiple_of(first, part), part), :]

    finals = []

    def send(t, name, src, dst, device, cond, w=None):
        n = index[name]
        out = n if w is None else len(names) + "XYD".index(w)

        def make():
            return pltpu.make_async_remote_copy(
                src_ref=view(t, src), dst_ref=view(t, dst),
                send_sem=send_sem.at[t, out], recv_sem=recv_sem.at[t, n],
                device_id=device, device_id_type=pl.DeviceIdType.MESH,
            )

        @pl.when(cond)
        def _():
            make().start()

        finals.append((cond, make))

    def pair_copy(t, name, start, sem_only=False):
        n = index[name]
        return pltpu.make_async_remote_copy(
            src_ref=view(t, start), dst_ref=view(t, start),
            send_sem=pair_send.at[t, n], recv_sem=pair_recv.at[t, n],
            device_id=partner, device_id_type=pl.DeviceIdType.MESH,
        )

    pair_waits = [[] for _ in range(2 * CHUNKS)]

    def arrive(t, name, start, other, cond):
        n = index[name]

        @pl.when(cond)
        def _():
            pltpu.make_async_remote_copy(
                src_ref=view(t, start), dst_ref=view(t, start),
                send_sem=send_sem.at[t, n], recv_sem=recv_sem.at[t, n],
                device_id=partner, device_id_type=pl.DeviceIdType.MESH,
            ).wait_recv()
            pair_copy(t, name, start).start()

        finals.append((cond, lambda: pair_copy(t, name, start)))
        pair_waits[t].append((cond, name, other))

    def both(start_of):
        return start_of(core), start_of(1 - core)

    def far(t, name, src, dst, step, cond):
        def make():
            return pltpu.make_async_remote_copy(
                src_ref=view(t, src), dst_ref=view(t, dst),
                send_sem=far_send.at[t, step], recv_sem=recv_sem.at[t, index[name]],
                device_id=dev(x, y, z + step, core), device_id_type=pl.DeviceIdType.MESH,
            )

        @pl.when(cond)
        def _():
            make().start()

        finals.append((cond, make))

    true = z >= 0

    def own_load(t):
        hbm = (k_hbm, v_hbm)[t // CHUNKS].at[pl.ds((t % CHUNKS) * part, part), :]
        return pltpu.make_async_copy(hbm, view(t, at(0, col)), local_sem.at[t])

    def own(t):
        own_load(t).wait()
        for w, device, other in ways:
            send(t, ("M", w), at(0, col), at(0, col), device, other > col)
        for d in range(1, reach + 1):
            far(t, ("Z", d), at(0, col), at(d, col) if d < reach else extra(0), d, z + d < planes)
        for d in range(reach + 1, planes):
            far(t, "S", at(0, col), extra(1), d, (z == 0) & (col == 0))
        pair_copy(t, "own", at(0, col)).start()
        finals.append((true, lambda: pair_copy(t, "own", at(0, col))))
        pair_waits[t].append((true, "own", at(0, col, 1 - core)))

    def column(t, d):
        start_of = (lambda cc: at(d, col, cc)) if d < reach else (lambda cc: extra(0, cc))
        here, other = both(start_of)
        arrive(t, ("Z", d), here, other, z >= d)
        for w, device, j in ways:
            if d < reach:
                send(t, ("F", d, w), here, here, device, z >= d)
            else:
                send(t, ("M", w), here, at(0, col), device, (z >= d) & (j < col))
                send(t, "S", here, extra(1), device, (z == d) & (col == 0), w)

    def column_sink(t):
        arrive(t, "S", *both(lambda cc: extra(1, cc)), (z > reach) & (col == 0))
        for w, device, j in ways:
            send(t, "S", extra(1), extra(1), device, (z > reach) & (col == 0), w)

    def mixed(t, late):
        for w, device, j in ways:
            cond = ((j > col) & (z >= reach)) if late else (j < col)
            arrive(t, ("M", w), *both(lambda cc, j=j: at(0, j, cc)), cond)

    def full(t, d):
        for w, device, j in ways:
            arrive(t, ("F", d, w), *both(lambda cc, j=j: at(d, j, cc)), z >= d)

    def sink(t):
        arrive(t, "S", *both(lambda cc: extra(1, cc)), (z >= reach) & (col > 0))

    def from_pair(t):
        for cond, name, other in pair_waits[t]:
            @pl.when(cond)
            def _():
                pair_copy(t, name, other).wait_recv()

    for t in range(2 * CHUNKS):
        own_load(t).start()
    q_copy = pltpu.make_async_copy(q_hbm, qbuf, local_sem.at[2 * CHUNKS])
    q_copy.start()
    lens_copy = pltpu.make_async_copy(lens_hbm, lens_ref, local_sem.at[2 * CHUNKS + 1])
    lens_copy.start()
    barrier = pltpu.get_barrier_semaphore()
    for device in (to_x, to_y, to_d, partner):
        pl.semaphore_signal(barrier, inc=1, device_id=device, device_id_type=pl.DeviceIdType.MESH)
    for step in range(1, planes):
        pl.semaphore_signal(
            barrier, inc=1, device_id=dev(x, y, (z + step) % planes, core),
            device_id_type=pl.DeviceIdType.MESH,
        )
    pl.semaphore_wait(barrier, planes + 3)

    for t in range(2 * CHUNKS):
        own(t)

    def clear(start, count, cond):
        @pl.when(cond)
        def _():
            for buf in bufs:
                buf[start:start + count, :] = jnp.zeros((count, buf.shape[1]), buf.dtype)

    for d in range(1, reach):
        clear(d * plane, plane, z < d)
    for j in range(1, 4):
        clear(j * chip, chip, (j > col) & (z < reach))
    clear(reach * plane, 2 * chip, z < reach)

    q_pos = ctx * (4 * rows) + kvh * rows + lax.broadcasted_iota(jnp.int32, (rows, 1), 0)
    first = jnp.zeros((rows, 1), jnp.int32)
    begin = jnp.int32(0)
    lens_copy.wait()
    for n in range(lens_ref.shape[0]):
        first = jnp.where(q_pos >= begin, begin, first)
        begin = begin + lens_ref[n]
    lane = lax.broadcasted_iota(jnp.int32, (1, chip), 1)

    def set_bias(start, base):
        k_pos = base + lane
        sees = (k_pos <= q_pos) & ((k_pos >= first) | ((k_pos < SINK) & (k_pos >= 0)))
        bias[:, start:start + chip] = jnp.where(sees, jnp.float32(0.0), jnp.float32(NEG))

    nowhere = -planes * plane * 2
    for j in range(4):
        set_bias(j * chip, jnp.where(j <= col, z, z - reach) * plane + j * chip)
        for d in range(1, reach):
            set_bias(d * plane + j * chip, (z - d) * plane + j * chip)
    set_bias(reach * plane, (z - reach) * plane + col * chip)
    set_bias(reach * plane + chip, jnp.where((z > reach) | ((z == reach) & (col > 0)), 0, nowhere))

    first_half, second_half = range(CHUNKS), range(CHUNKS, 2 * CHUNKS)

    def columns(ts):
        for d in range(1, reach + 1):
            for t in ts:
                column(t, d)
        for t in ts:
            column_sink(t)

    def early(ts):
        for t in ts:
            mixed(t, False)
        for d in range(1, reach):
            for t in ts:
                full(t, d)

    def final(ts):
        for t in ts:
            sink(t)
            mixed(t, True)
        for t in ts:
            from_pair(t)

    columns(first_half)
    columns(second_half)
    early(first_half)
    early(second_half)
    final(first_half)
    q_copy.wait()

    keys = bias.shape[1]
    step = 2 * chip
    tall = group * rows
    size = HEAD_SIZE

    def head_q(h):
        return jnp.concatenate(
            [qbuf[:, (h * group + g) * size:(h * group + g + 1) * size] for g in range(group)], axis=0
        )

    def fold(op, value, total):
        for n in range(value.shape[1] // size):
            total = op(total, value[:, n * size:(n + 1) * size])
        return total

    def each(body, init):
        count = keys // step
        if count <= 8:
            for n in range(count):
                init = body(n, init)
            return init
        return lax.fori_loop(0, count, body, init)

    def cut(n):
        return pl.ds(n * step if isinstance(n, int) else pl.multiple_of(n * step, step), step)

    tops = []
    for h in range(kv_heads):
        qh = head_q(h)

        def score(n, top, h=h, qh=qh):
            s = lax.dot_general(
                qh, kbuf[cut(n), h * size:(h + 1) * size], (((1,), (1,)), ((), ())),
                preferred_element_type=jnp.float32,
            )
            s = s + jnp.concatenate([bias[:, cut(n)]] * group, axis=0)
            scores[h * tall:(h + 1) * tall, cut(n)] = s
            return fold(jnp.maximum, s, top)

        top = each(score, jnp.full((tall, size), NEG, jnp.float32))
        tops.append(jnp.max(top, axis=1, keepdims=True))

    final(second_half)

    factor = jnp.float32(HEAD_SIZE ** -0.5 * math.log2(math.e))
    for h in range(kv_heads):
        def weigh(n, carry, h=h):
            total, acc = carry
            p = jnp.exp2((scores[h * tall:(h + 1) * tall, cut(n)] - tops[h]) * factor)
            acc = acc + jnp.dot(
                p.astype(jnp.bfloat16), vbuf[cut(n), h * size:(h + 1) * size],
                preferred_element_type=jnp.float32,
            )
            return fold(jnp.add, p, total), acc

        zero = jnp.zeros((tall, size), jnp.float32)
        total, acc = each(weigh, (zero, zero))
        out = (acc / jnp.sum(total, axis=1, keepdims=True)).astype(o_ref.dtype)
        for g in range(group):
            o_ref[:, (h * group + g) * size:(h * group + g + 1) * size] = out[g * rows:(g + 1) * rows]

    for cond, make in finals:
        @pl.when(cond)
        def _():
            make().wait_send()


def solution(mesh):
    planes = mesh.shape["ctx"] // 2
    reach = planes // 2

    def shards(queries, keys, values, doc_lengths):
        rows, width = keys.shape
        kv_heads = width // HEAD_SIZE
        group = queries.shape[1] // width
        span = (4 * reach + 2) * 2 * rows
        room = span * (4 * width + 4 * (kv_heads * group + 1) * rows) + 8 * queries.size
        pieces = 2 + reach + 3 * (reach - 1) + 3
        return pl.pallas_call(
            functools.partial(attention_kernel, planes, reach, kv_heads, group),
            out_shape=jax.ShapeDtypeStruct(queries.shape, queries.dtype),
            in_specs=[pl.BlockSpec(memory_space=pltpu.HBM)] * 4,
            out_specs=pl.BlockSpec(memory_space=pltpu.VMEM),
            scratch_shapes=[
                pltpu.SMEM(doc_lengths.shape, doc_lengths.dtype),
                pltpu.VMEM((span, width), keys.dtype),
                pltpu.VMEM((span, width), values.dtype),
                pltpu.VMEM(queries.shape, queries.dtype),
                pltpu.VMEM((kv_heads * group * rows, span), jnp.float32),
                pltpu.VMEM((rows, span), jnp.float32),
                pltpu.SemaphoreType.DMA((2 * CHUNKS + 2,)),
                pltpu.SemaphoreType.DMA((2 * CHUNKS, pieces + 3)),
                pltpu.SemaphoreType.DMA((2 * CHUNKS, pieces)),
                pltpu.SemaphoreType.DMA((2 * CHUNKS, pieces)),
                pltpu.SemaphoreType.DMA((2 * CHUNKS, pieces)),
                pltpu.SemaphoreType.DMA((2 * CHUNKS, planes)),
            ],
            compiler_params=pltpu.CompilerParams(
                collective_id=0, has_side_effects=True, vmem_limit_bytes=min(room + 3 * 1024 * 1024, 64 * 1024 * 1024 - 65536),
            ),
            name="attend",
        )(*[pltpu.with_memory_space_constraint(a, pltpu.HBM) for a in (doc_lengths, queries, keys, values)])

    placed = (P(("ctx", "kvh"), None), P(("ctx", "kvh"), None), P(("ctx", "kvh"), None), P())
    return jax.shard_map(
        shards, mesh=mesh, in_specs=placed, out_specs=P(("ctx", "kvh"), None), check_vma=False
    )
```
